128 devices in a mesh: row: 4 (over z_lo, core), col: 32 (over z_hi, y, x).
Axes of the slice: x: 4, y: 4, z: 4 (z_hi: 2, z_lo: 2; z = z_hi * 2 + z_lo), core: 2. Of those that a mesh axis runs over, the one named last changes fastest.
Arguments:
- left_factor: bfloat16 [4096, 8192], P('row', 'col'), may hold values from -6 to 6
- right_factor: bfloat16 [8192, 32768], P('row', 'col'), may hold values from -0.0625 to 0.0625
- matrix: float32 [4096, 32768], P('row', 'col'), may hold values from -6 to 6
- pivot_scale: float32 [8192], replicated, may hold values from 0.25 to 1.75
Outputs:
- updated: float32 [4096, 32768], P('row', 'col')
The draws below stay inside these ranges and needn't reach their ends.
All inputs are finite; a program needn't handle non-finite values.
Results may differ from the reference program's by a relative error of at most 0.0003.
Values may be sent and summed in bfloat16 or wider, within the bound.
A program may use at most 128 MiB of HBM per device.

```python
import jax
import jax.numpy as jnp
from jax import lax

ROWS = 4096
COLS = 32768
INNER = 8192


def levels(rng, shape, split, least, top_value):
    def one(position, blocks):
        draws = jax.random.uniform(jax.random.fold_in(jax.random.fold_in(rng, 6), position), (blocks,), jnp.float32, least / len(split), top_value / len(split))
        return jnp.repeat(jnp.exp(draws), shape[position] // blocks).reshape((-1,) + (1,) * (len(shape) - position - 1))

    factor_of = one(*split[0])
    for cut in split[1:]:
        factor_of = factor_of * one(*cut)
    return factor_of


def scatter_about(stream_key, shape, spread, reach, split=(), held_as=jnp.bfloat16):
    gain = levels(stream_key, shape, split, -0.22, 0.18) if split else 1.0
    array = jax.random.normal(stream_key, shape, jnp.float32) * spread * gain
    return jnp.minimum(jnp.maximum(array, -reach), reach).astype(held_as)


def setup_inputs(seed: int = 0) -> dict:
    key_list = jax.random.split(jax.random.key(seed), 5)
    return {
        "left_factor": scatter_about(key_list[0], (ROWS, INNER), 1.0, 6.0, ((0, 4), (1, 32))),
        "right_factor": scatter_about(key_list[1], (INNER, COLS), INNER ** -0.5, 0.0625, ((0, 4), (1, 32))),
        "matrix": scatter_about(key_list[2], (ROWS, COLS), 1.0, 6.0, ((0, 4), (1, 32)), jnp.float32),
        "pivot_scale": jnp.clip(1.0 + 0.15 * jax.random.normal(key_list[3], (INNER,), jnp.float32), 0.25, 1.75),
    }


def reference(left_factor, right_factor, matrix, pivot_scale):
    scaled_left = (left_factor.astype(jnp.float32) * pivot_scale).astype(jnp.bfloat16)
    updated = matrix - jnp.dot(scaled_left, right_factor, preferred_element_type=jnp.float32)
    row_power = lax.optimization_barrier(jnp.sum(updated * updated, axis=1))
    updated = updated * lax.rsqrt(row_power / COLS + 1e-06)[:, None]
    return updated
```

```python
import jax
import jax.numpy as jnp
from jax import lax
from jax.experimental import pallas as pl
from jax.experimental.pallas import tpu as pltpu
from jax.sharding import Mesh
from jax.sharding import PartitionSpec as P

MESH = pl.DeviceIdType.MESH
ROW = ("zl", "core")
COL = ("zh", "y", "x")
STAGES = 4
R = 256
HALF = R // 2
DEPTH = 256
OFFSETS = (0, -1, 1, 2)


def encode(v):
    t = v * 16.0
    t2 = t * t
    t4 = t2 * t2
    t8 = t4 * t4
    return jnp.where(t < 0.0, -t8, t8).astype(jnp.bfloat16)


def decode(c):
    y = c.astype(jnp.float32)
    r = jnp.sqrt(jnp.sqrt(jnp.sqrt(jnp.abs(y)))) * 0.0625
    return jnp.where(y < 0.0, -r, r)


def kernel(
    left, right, matrix, out, power,
    buf, bk, acc, csend, crecv, sx, sy, sz,
    send_sem, recv_sem, z_send, z_recv, c_send, c_recv, n_send, n_recv, b_send, b_recv, local_sem,
):
    x, y = lax.axis_index("x"), lax.axis_index("y")
    zl, zh, core = lax.axis_index("zl"), lax.axis_index("zh"), lax.axis_index("core")
    at = {"x": x, "y": y}
    mine = y * 4 + x

    own_b = pltpu.make_async_copy(right, bk.at[pl.ds(core * 8, 8)], local_sem.at[0])
    own_m = pltpu.make_async_copy(matrix, acc.at[pl.ds(4, 4)], local_sem.at[1])
    own_b.start()
    own_m.start()

    barrier = pltpu.get_barrier_semaphore()
    peers = [{"core": 1 - core}]
    for d in (1, 2, 3):
        peers.append({"x": lax.rem(x + d, 4)})
        peers.append({"y": lax.rem(y + d, 4)})
    peers.append({"zl": 1 - zl})
    peers.append({"zh": 1 - zh})
    peers.append({"zl": 1 - zl, "zh": 1 - zh})
    for peer in peers:
        pl.semaphore_signal(barrier, inc=1, device_id=peer, device_id_type=MESH)
    for i in range(4):
        acc[i] = jnp.zeros((R, acc.shape[2]), jnp.float32)
    pl.semaphore_wait(barrier, len(peers))

    def z_copy(sub, c, stage, zh_to, k):
        return pltpu.make_async_remote_copy(
            src_ref=left.at[sub, c], dst_ref=buf.at[stage, mine, c],
            send_sem=z_send.at[k, sub, c], recv_sem=z_recv.at[stage, c],
            device_id={"zl": zh, "zh": zh_to}, device_id_type=MESH,
        )

    inner = zh != zl

    @pl.when(inner)
    def _():
        for sub in range(2):
            for c in range(2):
                z_copy(sub, c, sub, 0, 0).start()
                z_copy(sub, c, sub, 1, 1).start()

    other_b = pltpu.make_async_remote_copy(
        src_ref=right, dst_ref=bk.at[pl.ds(core * 8, 8)],
        send_sem=b_send, recv_sem=b_recv, device_id={"core": 1 - core}, device_id_type=MESH,
    )
    other_b.start()

    def spot(c, dp, ds):
        px, py = (dp, ds) if c == 0 else (ds, dp)
        return lax.rem(y + py + 4, 4) * 4 + lax.rem(x + px + 4, 4)

    def hop(s, c, event, first, step, j, part):
        axis = "xy"[c] if first else "xy"[1 - c]
        rows = (slice(None), pl.ds(0, HALF), pl.ds(HALF, HALF))[part]
        piece = buf.at[s, j, c, rows]
        return pltpu.make_async_remote_copy(
            src_ref=piece, dst_ref=piece,
            send_sem=send_sem.at[s, c, event], recv_sem=recv_sem.at[s, c, event],
            device_id={axis: lax.rem(at[axis] + step + 4, 4)}, device_id_type=MESH,
        )

    def multiply(s, c, j):
        acc[2 * s + c] -= jnp.dot(buf[s, j, c], bk[j], preferred_element_type=jnp.float32)

    def send_column(s, c, k):
        j = spot(c, OFFSETS[k], 0)
        hop(s, c, 4 + 4 * k, False, 1, j, 0).start()
        hop(s, c, 5 + 4 * k, False, -1, j, 0).start()

    def begin(s):
        for c in range(2):
            pltpu.make_async_copy(left.at[0, 0], buf.at[s, mine, c], z_recv.at[s, c]).wait()
            hop(s, c, 0, True, 1, mine, 0).start()
            hop(s, c, 1, True, -1, mine, 0).start()
            send_column(s, c, 0)

    def first_near(s, c):
        for e, step in ((0, 1), (1, -1)):
            j = spot(c, -step, 0)
            hop(s, c, e, True, step, j, 0).wait_recv()
            hop(s, c, 2 + e, True, step, j, 1 + e).start()
            send_column(s, c, 1 + e)
            multiply(s, c, j)

    def first_far(s, c):
        j = spot(c, 2, 0)
        hop(s, c, 2, True, 1, j, 1).wait_recv()
        hop(s, c, 3, True, -1, j, 2).wait_recv()
        send_column(s, c, 3)
        multiply(s, c, j)

    def second_near(s, c, k):
        for e, step in ((0, 1), (1, -1)):
            j = spot(c, OFFSETS[k], -step)
            hop(s, c, 4 + 4 * k + e, False, step, j, 0).wait_recv()
            hop(s, c, 6 + 4 * k + e, False, step, j, 1 + e).start()
            multiply(s, c, j)

    def second_far(s, c, k):
        j = spot(c, OFFSETS[k], 2)
        hop(s, c, 6 + 4 * k, False, 1, j, 1).wait_recv()
        hop(s, c, 7 + 4 * k, False, -1, j, 2).wait_recv()
        multiply(s, c, j)

    def part_copy(i):
        return pltpu.make_async_remote_copy(
            src_ref=csend.at[i], dst_ref=crecv.at[i],
            send_sem=c_send.at[i], recv_sem=c_recv.at[i],
            device_id={"zl": 1 - zl}, device_id_type=MESH,
        )

    def fold(i):
        part_copy(i).wait_recv()
        acc[4 + i] += decode(crecv[i])

    @pl.loop(0, STAGES + 1)
    def _(s):
        fresh = s < STAGES
        old = s - 1

        @pl.when(fresh)
        def _():
            begin(s)

        @pl.when(jnp.logical_and(s == 0, jnp.logical_not(inner)))
        def _():
            for sub in range(2):
                for c in range(2):
                    pltpu.make_async_copy(
                        left.at[sub, c], buf.at[2 + sub, mine, c], z_recv.at[2 + sub, c]
                    ).start()
                    z_copy(sub, c, 2 + sub, 1 - zh, 0).start()

        @pl.when(s == 0)
        def _():
            own_b.wait()
            own_m.wait()
            other_b.wait_recv()

        @pl.when(s > 0)
        def _():
            for k in range(3):
                for c in (1, 0):
                    second_far(old, c, k)
            for c in (1, 0):
                second_near(old, c, 3)

        @pl.when(fresh)
        def _():
            for c in range(2):
                multiply(s, c, mine)
            for c in range(2):
                first_near(s, c)
            for c in (1, 0):
                second_near(s, c, 0)

        @pl.when(s > 0)
        def _():
            for c in (1, 0):
                second_far(old, c, 3)

        @pl.when(jnp.logical_and(s > 0, s < 3))
        def _():
            for c in range(2):
                csend[2 * old + c] = encode(acc[2 * old + c])
            for c in range(2):
                part_copy(2 * old + c).start()

        @pl.when(s == STAGES - 1)
        def _():
            for i in range(4):
                fold(i)

        @pl.when(fresh)
        def _():
            first_far(s, 0)
            for k in (1, 2):
                for c in range(2):
                    second_near(s, c, k)
            first_far(s, 1)

    own_out = pltpu.make_async_copy(acc.at[pl.ds(4, 4)], out, local_sem.at[0])
    own_out.start()
    for i in range(4):
        u = acc[4 + i]
        u = u * u
        t = u[:, :128]
        for j in range(1, u.shape[1] // 128):
            t = t + u[:, j * 128:(j + 1) * 128]
        sx[x, i] = jnp.sum(t.T, axis=0)

    def exchange(phase, slots, axis, me, n):
        def to(d):
            return pltpu.make_async_remote_copy(
                src_ref=slots.at[me], dst_ref=slots.at[me],
                send_sem=n_send.at[phase, d], recv_sem=n_recv.at[phase, d],
                device_id={axis: lax.rem(me + d, n)}, device_id_type=MESH,
            )

        for d in range(1, n):
            to(d).start()
        for d in range(1, n):
            came = slots.at[lax.rem(me - d + n, n)]
            pltpu.make_async_remote_copy(
                src_ref=came, dst_ref=came,
                send_sem=n_send.at[phase, d], recv_sem=n_recv.at[phase, d],
                device_id={axis: lax.rem(me + d, n)}, device_id_type=MESH,
            ).wait_recv()
        total = slots[0]
        for d in range(1, n):
            total = total + slots[d]
        return total

    sy[y] = exchange(0, sx, "x", x, 4)
    sz[zh] = exchange(1, sy, "y", y, 4)
    power[...] = exchange(2, sz, "zh", zh, 2)

    for phase, slots, axis, me, n in ((0, sx, "x", x, 4), (1, sy, "y", y, 4), (2, sz, "zh", zh, 2)):
        for d in range(1, n):
            pltpu.make_async_remote_copy(
                src_ref=slots.at[me], dst_ref=slots.at[me],
                send_sem=n_send.at[phase, d], recv_sem=n_recv.at[phase, d],
                device_id={axis: lax.rem(me + d, n)}, device_id_type=MESH,
            ).wait_send()
    for i in range(4):
        part_copy(i).wait_send()
    other_b.wait_send()

    @pl.when(inner)
    def _():
        for sub in range(2):
            for c in range(2):
                z_copy(sub, c, sub, 0, 0).wait_send()
                z_copy(sub, c, sub, 1, 1).wait_send()

    @pl.when(jnp.logical_not(inner))
    def _():
        for sub in range(2):
            for c in range(2):
                z_copy(sub, c, 2 + sub, 1 - zh, 0).wait_send()

    @pl.loop(0, STAGES)
    def _(s):
        for c in range(2):
            for e in range(20):
                far = e % 4 >= 2
                hop(s, c, e, True, 1, mine, 1 if far else 0).wait_send()
    own_out.wait()


def body(left_factor, right_factor, matrix, pivot_scale):
    share = left_factor.shape[1]
    part_scale = lax.dynamic_slice_in_dim(pivot_scale, lax.axis_index(COL) * share, share)
    scaled_left = (left_factor.astype(jnp.float32) * part_scale).astype(jnp.bfloat16)
    columns = matrix.shape[1]
    dma = pltpu.SemaphoreType.DMA
    updated, power = pl.pallas_call(
        kernel,
        out_shape=(
            jax.ShapeDtypeStruct((4, R, columns), jnp.float32),
            jax.ShapeDtypeStruct((4, R), jnp.float32),
        ),
        in_specs=[pl.BlockSpec(memory_space=pl.ANY)] * 3,
        out_specs=(pl.BlockSpec(memory_space=pl.ANY), pl.BlockSpec(memory_space=pltpu.VMEM)),
        scratch_shapes=[
            pltpu.VMEM((STAGES, 16, 2, R, DEPTH), jnp.bfloat16),
            pltpu.VMEM((16, DEPTH, columns), jnp.bfloat16),
            pltpu.VMEM((8, R, columns), jnp.float32),
            pltpu.VMEM((4, R, columns), jnp.bfloat16),
            pltpu.VMEM((4, R, columns), jnp.bfloat16),
            pltpu.VMEM((4, 4, R), jnp.float32),
            pltpu.VMEM((4, 4, R), jnp.float32),
            pltpu.VMEM((2, 4, R), jnp.float32),
            dma((STAGES, 2, 20)),
            dma((STAGES, 2, 20)),
            dma((2, 2, 2)),
            dma((STAGES, 2)),
            dma((4,)),
            dma((4,)),
            dma((3, 4)),
            dma((3, 4)),
            dma,
            dma,
            dma((2,)),
        ],
        compiler_params=pltpu.CompilerParams(collective_id=0, has_side_effects=True, vmem_limit_bytes=46 * 2**20),
        name="update",
    )(
        scaled_left.reshape(2, 2, R, DEPTH),
        right_factor.reshape(8, DEPTH, columns),
        matrix.reshape(4, R, columns),
    )
    updated = updated.reshape(matrix.shape)
    row_power = power.reshape(matrix.shape[0])
    return updated * lax.rsqrt(row_power / (columns * 32) + 1e-06)[:, None]


def solution(mesh):
    torus = Mesh(mesh.devices.reshape(2, 2, 2, 4, 4), ROW + COL)
    in_specs = (P(ROW, COL), P(ROW, COL), P(ROW, COL), P())
    return jax.shard_map(body, mesh=torus, in_specs=in_specs, out_specs=P(ROW, COL), check_vma=False)
```

```python
import jax
import jax.numpy as jnp
from jax import lax
from jax.experimental import pallas as pl
from jax.experimental.pallas import tpu as pltpu
from jax.sharding import Mesh
from jax.sharding import PartitionSpec as P

MESH = pl.DeviceIdType.MESH
ROW = ("zl", "core")
COL = ("zh", "y", "x")
STAGES = 4
R = 256
HALF = R // 2
DEPTH = 256
OFFSETS = (0, -1, 1, 2)


def encode(v):
    t = v * 16.0
    t2 = t * t
    t4 = t2 * t2
    t8 = t4 * t4
    return jnp.where(t < 0.0, -t8, t8).astype(jnp.bfloat16)


def decode(c):
    y = c.astype(jnp.float32)
    r = jnp.sqrt(jnp.sqrt(jnp.sqrt(jnp.abs(y)))) * 0.0625
    return jnp.where(y < 0.0, -r, r)


def kernel(
    raw, scales, right, matrix, out, power,
    fresh_left, scale_rows, left, buf, bk, acc, csend, crecv, sums,
    send_sem, recv_sem, z_send, z_recv, c_send, c_recv, n_send, n_recv, b_send, b_recv, local_sem,
):
    x, y = lax.axis_index("x"), lax.axis_index("y")
    zl, zh, core = lax.axis_index("zl"), lax.axis_index("zh"), lax.axis_index("core")
    at = {"x": x, "y": y}
    mine = y * 4 + x

    own_b = pltpu.make_async_copy(right, bk.at[pl.ds(core * 8, 8)], local_sem.at[0])
    own_m = pltpu.make_async_copy(matrix, acc.at[pl.ds(4, 4)], local_sem.at[1])
    own_left = pltpu.make_async_copy(raw, fresh_left, local_sem.at[4])
    own_scales = pltpu.make_async_copy(scales, scale_rows, local_sem.at[5])
    own_left.start()
    own_scales.start()
    own_b.start()
    own_m.start()

    barrier = pltpu.get_barrier_semaphore()
    peers = [{"core": 1 - core}]
    for d in (1, 2, 3):
        peers.append({"x": lax.rem(x + d, 4)})
        peers.append({"y": lax.rem(y + d, 4)})
    peers.append({"zl": 1 - zl})
    peers.append({"zh": 1 - zh})
    peers.append({"zl": 1 - zl, "zh": 1 - zh})
    for peer in peers:
        pl.semaphore_signal(barrier, inc=1, device_id=peer, device_id_type=MESH)
    for i in range(4):
        acc[i] = jnp.zeros((R, acc.shape[2]), jnp.float32)
    own_scales.wait()
    own_left.wait()
    chunk = (zh * 16 + mine) * 2
    for part in range(2):
        columns = slice(part * 128, (part + 1) * 128)
        scale = scale_rows[pl.ds(chunk + part, 1), :]
        for sub in range(2):
            for c in range(2):
                left[sub, c, :, columns] = (
                    fresh_left[sub, c, :, columns].astype(jnp.float32) * scale
                ).astype(jnp.bfloat16)
    pl.semaphore_wait(barrier, len(peers))

    def z_copy(sub, c, stage, zh_to, k):
        return pltpu.make_async_remote_copy(
            src_ref=left.at[sub, c], dst_ref=buf.at[stage, mine, c],
            send_sem=z_send.at[k, sub, c], recv_sem=z_recv.at[stage, c],
            device_id={"zl": zh, "zh": zh_to}, device_id_type=MESH,
        )

    inner = zh != zl

    @pl.when(inner)
    def _():
        for sub in range(2):
            for c in range(2):
                z_copy(sub, c, sub, 0, 0).start()
                z_copy(sub, c, sub, 1, 1).start()

    other_b = pltpu.make_async_remote_copy(
        src_ref=right, dst_ref=bk.at[pl.ds(core * 8, 8)],
        send_sem=b_send, recv_sem=b_recv, device_id={"core": 1 - core}, device_id_type=MESH,
    )
    other_b.start()

    def spot(c, dp, ds):
        px, py = (dp, ds) if c == 0 else (ds, dp)
        return lax.rem(y + py + 4, 4) * 4 + lax.rem(x + px + 4, 4)

    def hop(s, c, event, first, step, j, part):
        axis = "xy"[c] if first else "xy"[1 - c]
        rows = (slice(None), pl.ds(0, HALF), pl.ds(HALF, HALF))[part]
        piece = buf.at[s, j, c, rows]
        return pltpu.make_async_remote_copy(
            src_ref=piece, dst_ref=piece,
            send_sem=send_sem.at[s, c, event], recv_sem=recv_sem.at[s, c, event],
            device_id={axis: lax.rem(at[axis] + step + 4, 4)}, device_id_type=MESH,
        )

    def multiply(s, c, j):
        acc[2 * s + c] -= jnp.dot(buf[s, j, c], bk[j], preferred_element_type=jnp.float32)

    def send_column(s, c, k):
        j = spot(c, OFFSETS[k], 0)
        hop(s, c, 4 + 4 * k, False, 1, j, 0).start()
        hop(s, c, 5 + 4 * k, False, -1, j, 0).start()

    def begin(s):
        for c in range(2):
            pltpu.make_async_copy(left.at[0, 0], buf.at[s, mine, c], z_recv.at[s, c]).wait()
            hop(s, c, 0, True, 1, mine, 0).start()
            hop(s, c, 1, True, -1, mine, 0).start()
            send_column(s, c, 0)

    def first_near(s, c):
        for e, step in ((0, 1), (1, -1)):
            j = spot(c, -step, 0)
            hop(s, c, e, True, step, j, 0).wait_recv()
            hop(s, c, 2 + e, True, step, j, 1 + e).start()
            send_column(s, c, 1 + e)
            multiply(s, c, j)

    def first_far(s, c):
        j = spot(c, 2, 0)
        hop(s, c, 2, True, 1, j, 1).wait_recv()
        hop(s, c, 3, True, -1, j, 2).wait_recv()
        send_column(s, c, 3)
        multiply(s, c, j)

    def second_near(s, c, k):
        for e, step in ((0, 1), (1, -1)):
            j = spot(c, OFFSETS[k], -step)
            hop(s, c, 4 + 4 * k + e, False, step, j, 0).wait_recv()
            hop(s, c, 6 + 4 * k + e, False, step, j, 1 + e).start()
            multiply(s, c, j)

    def second_far(s, c, k):
        j = spot(c, OFFSETS[k], 2)
        hop(s, c, 6 + 4 * k, False, 1, j, 1).wait_recv()
        hop(s, c, 7 + 4 * k, False, -1, j, 2).wait_recv()
        multiply(s, c, j)

    def part_copy(i):
        return pltpu.make_async_remote_copy(
            src_ref=csend.at[i], dst_ref=crecv.at[i],
            send_sem=c_send.at[i], recv_sem=c_recv.at[i],
            device_id={"zl": 1 - zl}, device_id_type=MESH,
        )

    def fold(i):
        part_copy(i).wait_recv()
        acc[4 + i] += decode(crecv[i])

    place = (zh * 4 + y) * 4 + x

    def power_copy(d):
        dz, dy, dx = d // 16, d // 4 % 4, d % 4
        return pltpu.make_async_remote_copy(
            src_ref=sums.at[place], dst_ref=sums.at[place],
            send_sem=n_send.at[d], recv_sem=n_recv.at[d],
            device_id={
                "zh": lax.rem(zh + dz, 2), "y": lax.rem(y + dy, 4), "x": lax.rem(x + dx, 4)
            },
            device_id_type=MESH,
        )

    def out_copy(half):
        return pltpu.make_async_copy(
            acc.at[pl.ds(4 + 2 * half, 2)], out.at[pl.ds(2 * half, 2)], local_sem.at[2 + half]
        )

    def square(i):
        u = acc[4 + i]
        u = u * u
        t = u[:, :128]
        for j in range(1, u.shape[1] // 128):
            t = t + u[:, j * 128:(j + 1) * 128]
        sums[place, i] = jnp.sum(t.T, axis=0)

    @pl.loop(0, STAGES + 1)
    def _(s):
        fresh = s < STAGES
        old = s - 1

        @pl.when(fresh)
        def _():
            begin(s)

        @pl.when(jnp.logical_and(s == 0, jnp.logical_not(inner)))
        def _():
            for sub in range(2):
                for c in range(2):
                    pltpu.make_async_copy(
                        left.at[sub, c], buf.at[2 + sub, mine, c], z_recv.at[2 + sub, c]
                    ).start()
                    z_copy(sub, c, 2 + sub, 1 - zh, 0).start()

        @pl.when(s == 0)
        def _():
            own_b.wait()
            own_m.wait()
            other_b.wait_recv()

        @pl.when(s > 0)
        def _():
            for k in range(3):
                for c in (1, 0):
                    second_far(old, c, k)
            for c in (1, 0):
                second_near(old, c, 3)

        @pl.when(fresh)
        def _():
            for c in range(2):
                multiply(s, c, mine)
            for c in range(2):
                first_near(s, c)
            for c in (1, 0):
                second_near(s, c, 0)

        @pl.when(s > 0)
        def _():
            for c in (1, 0):
                second_far(old, c, 3)

        @pl.when(jnp.logical_and(s > 0, s < 3))
        def _():
            for c in range(2):
                csend[2 * old + c] = encode(acc[2 * old + c])
            for c in range(2):
                part_copy(2 * old + c).start()

        @pl.when(s == STAGES - 1)
        def _():
            for i in range(4):
                fold(i)
            for i in range(2):
                square(i)
            out_copy(0).start()

        @pl.when(fresh)
        def _():
            first_far(s, 0)
            for k in (1, 2):
                for c in range(2):
                    second_near(s, c, k)
            first_far(s, 1)

    for i in (2, 3):
        square(i)
    out_copy(1).start()
    for d in range(31, 0, -1):
        power_copy(d).start()
    for d in range(1, 32):
        power_copy(d).wait_recv()
    total = sums[0]
    for d in range(1, 32):
        total = total + sums[d]
    power[...] = total

    for d in range(1, 32):
        power_copy(d).wait_send()
    for i in range(4):
        part_copy(i).wait_send()
    other_b.wait_send()

    @pl.when(inner)
    def _():
        for sub in range(2):
            for c in range(2):
                z_copy(sub, c, sub, 0, 0).wait_send()
                z_copy(sub, c, sub, 1, 1).wait_send()

    @pl.when(jnp.logical_not(inner))
    def _():
        for sub in range(2):
            for c in range(2):
                z_copy(sub, c, 2 + sub, 1 - zh, 0).wait_send()

    @pl.loop(0, STAGES)
    def _(s):
        for c in range(2):
            for e in range(20):
                far = e % 4 >= 2
                hop(s, c, e, True, 1, mine, 1 if far else 0).wait_send()
    out_copy(0).wait()
    out_copy(1).wait()


def body(left_factor, right_factor, matrix, pivot_scale):
    columns = matrix.shape[1]
    dma = pltpu.SemaphoreType.DMA
    updated, power = pl.pallas_call(
        kernel,
        out_shape=(
            jax.ShapeDtypeStruct((4, R, columns), jnp.float32),
            jax.ShapeDtypeStruct((4, R), jnp.float32),
        ),
        in_specs=[pl.BlockSpec(memory_space=pl.ANY)] * 4,
        out_specs=(pl.BlockSpec(memory_space=pl.ANY), pl.BlockSpec(memory_space=pltpu.VMEM)),
        scratch_shapes=[
            pltpu.VMEM((2, 2, R, DEPTH), jnp.bfloat16),
            pltpu.VMEM((64, 128), jnp.float32),
            pltpu.VMEM((2, 2, R, DEPTH), jnp.bfloat16),
            pltpu.VMEM((STAGES, 16, 2, R, DEPTH), jnp.bfloat16),
            pltpu.VMEM((16, DEPTH, columns), jnp.bfloat16),
            pltpu.VMEM((8, R, columns), jnp.float32),
            pltpu.VMEM((4, R, columns), jnp.bfloat16),
            pltpu.VMEM((4, R, columns), jnp.bfloat16),
            pltpu.VMEM((32, 4, R), jnp.float32),
            dma((STAGES, 2, 20)),
            dma((STAGES, 2, 20)),
            dma((2, 2, 2)),
            dma((STAGES, 2)),
            dma((4,)),
            dma((4,)),
            dma((32,)),
            dma((32,)),
            dma,
            dma,
            dma((6,)),
        ],
        compiler_params=pltpu.CompilerParams(collective_id=0, has_side_effects=True, vmem_limit_bytes=46 * 2**20),
        name="update",
    )(
        pltpu.with_memory_space_constraint(left_factor.reshape(2, 2, R, DEPTH), pltpu.HBM),
        pltpu.with_memory_space_constraint(pivot_scale.reshape(64, 128), pltpu.HBM),
        right_factor.reshape(8, DEPTH, columns),
        matrix.reshape(4, R, columns),
    )
    updated = updated.reshape(matrix.shape)
    row_power = power.reshape(matrix.shape[0])
    return updated * lax.rsqrt(row_power / (columns * 32) + 1e-06)[:, None]


def solution(mesh):
    torus = Mesh(mesh.devices.reshape(2, 2, 2, 4, 4), ROW + COL)
    in_specs = (P(ROW, COL), P(ROW, COL), P(ROW, COL), P())
    return jax.shard_map(body, mesh=torus, in_specs=in_specs, out_specs=P(ROW, COL), check_vma=False)
```

```python
import jax
import jax.numpy as jnp
from jax import lax
from jax.experimental import pallas as pl
from jax.experimental.pallas import tpu as pltpu
from jax.sharding import Mesh
from jax.sharding import PartitionSpec as P

MESH = pl.DeviceIdType.MESH
ROW = ("zl", "core")
COL = ("zh", "y", "x")
STAGES = 4
R = 256
HALF = R // 2
DEPTH = 256
HALVES = (pl.ds(0, HALF), pl.ds(HALF, HALF))
OFFSETS = (0, -1, 1, 2)


def encode(v):
    t = v * 16.0
    t2 = t * t
    t4 = t2 * t2
    t8 = t4 * t4
    return jnp.where(t < 0.0, -t8, t8).astype(jnp.bfloat16)


def decode(c):
    y = c.astype(jnp.float32)
    r = jnp.exp2(jnp.log2(jnp.abs(y)) * 0.125 - 4.0)
    return jnp.where(y < 0.0, -r, r)


def kernel(
    raw, scales, right, matrix, out, power,
    fresh_left, scale_rows, left, buf, bk, acc, csend, crecv, sums,
    send_sem, recv_sem, z_send, z_recv, c_send, c_recv, n_send, n_recv, b_send, b_recv, local_sem,
):
    x, y = lax.axis_index("x"), lax.axis_index("y")
    zl, zh, core = lax.axis_index("zl"), lax.axis_index("zh"), lax.axis_index("core")
    at = {"x": x, "y": y}
    mine = y * 4 + x

    own_b = pltpu.make_async_copy(right, bk.at[pl.ds(core * 8, 8)], local_sem.at[0])
    own_m = pltpu.make_async_copy(matrix, acc.at[pl.ds(4, 4)], local_sem.at[1])
    own_left = pltpu.make_async_copy(raw, fresh_left, local_sem.at[4])
    own_scales = pltpu.make_async_copy(scales, scale_rows, local_sem.at[5])
    own_left.start()
    own_scales.start()
    own_b.start()
    own_m.start()

    barrier = pltpu.get_barrier_semaphore()
    peers = [{"core": 1 - core}]
    for d in (1, 3):
        peers.append({"x": lax.rem(x + d, 4)})
        peers.append({"y": lax.rem(y + d, 4)})
        z = lax.rem(2 * zh + zl + d, 4)
        peers.append({"zh": z // 2, "zl": lax.rem(z, 2)})
    for peer in peers:
        pl.semaphore_signal(barrier, inc=1, device_id=peer, device_id_type=MESH)
    for i in range(4):
        acc[i] = jnp.zeros((R, acc.shape[2]), jnp.float32)
    own_scales.wait()
    own_left.wait()
    chunk = (zh * 16 + mine) * 2
    for part in range(2):
        columns = slice(part * 128, (part + 1) * 128)
        scale = scale_rows[pl.ds(chunk + part, 1), :]
        for sub in range(2):
            for c in range(2):
                left[sub, c, :, columns] = (
                    fresh_left[sub, c, :, columns].astype(jnp.float32) * scale
                ).astype(jnp.bfloat16)
    pl.semaphore_wait(barrier, len(peers))

    def z_copy(sub, c, p, stage, zh_to, k):
        return pltpu.make_async_remote_copy(
            src_ref=left.at[sub, c, HALVES[p]], dst_ref=buf.at[stage, mine, c, HALVES[p]],
            send_sem=z_send.at[k, sub, c, p], recv_sem=z_recv.at[stage, c, p],
            device_id={"zl": zh, "zh": zh_to}, device_id_type=MESH,
        )

    inner = zh != zl

    @pl.when(inner)
    def _():
        for sub in range(2):
            for c in range(2):
                for p in range(2):
                    z_copy(sub, c, p, sub, 0, 0).start()
                    z_copy(sub, c, p, sub, 1, 1).start()

    other_b = pltpu.make_async_remote_copy(
        src_ref=right, dst_ref=bk.at[pl.ds(core * 8, 8)],
        send_sem=b_send, recv_sem=b_recv, device_id={"core": 1 - core}, device_id_type=MESH,
    )
    other_b.start()

    def spot(c, dp, ds):
        px, py = (dp, ds) if c == 0 else (ds, dp)
        return lax.rem(y + py + 4, 4) * 4 + lax.rem(x + px + 4, 4)

    def hop(s, c, event, first, step, j, part):
        axis = "xy"[c] if first else "xy"[1 - c]
        rows = (slice(None), pl.ds(0, HALF), pl.ds(HALF, HALF))[part]
        piece = buf.at[s, j, c, rows]
        return pltpu.make_async_remote_copy(
            src_ref=piece, dst_ref=piece,
            send_sem=send_sem.at[s, c, event], recv_sem=recv_sem.at[s, c, event],
            device_id={axis: lax.rem(at[axis] + step + 4, 4)}, device_id_type=MESH,
        )

    def multiply(s, c, j):
        acc[2 * s + c] -= jnp.dot(buf[s, j, c], bk[j], preferred_element_type=jnp.float32)

    def send_column(s, c, k):
        j = spot(c, OFFSETS[k], 0)
        hop(s, c, 4 + 4 * k, False, 1, j, 0).start()
        hop(s, c, 5 + 4 * k, False, -1, j, 0).start()

    def begin(s):
        for c in range(2):
            for p in range(2):
                pltpu.make_async_copy(
                    left.at[0, 0, HALVES[0]], buf.at[s, mine, c, HALVES[p]], z_recv.at[s, c, p]
                ).wait()
                hop(s, c, 0, True, 1, mine, 1 + p).start()
                hop(s, c, 1, True, -1, mine, 1 + p).start()
                hop(s, c, 4, False, 1, mine, 1 + p).start()
                hop(s, c, 5, False, -1, mine, 1 + p).start()

    def first_near(s, c):
        for e, step in ((0, 1), (1, -1)):
            j = spot(c, -step, 0)
            hop(s, c, e, True, step, j, 0).wait_recv()
            hop(s, c, 2 + e, True, step, j, 1 + e).start()
            send_column(s, c, 1 + e)
            multiply(s, c, j)

    def first_far(s, c):
        j = spot(c, 2, 0)
        hop(s, c, 2, True, 1, j, 1).wait_recv()
        hop(s, c, 3, True, -1, j, 2).wait_recv()
        send_column(s, c, 3)
        multiply(s, c, j)

    def second_near(s, c, k):
        for e, step in ((0, 1), (1, -1)):
            j = spot(c, OFFSETS[k], -step)
            hop(s, c, 4 + 4 * k + e, False, step, j, 0).wait_recv()
            hop(s, c, 6 + 4 * k + e, False, step, j, 1 + e).start()
            multiply(s, c, j)

    def second_far(s, c, k):
        j = spot(c, OFFSETS[k], 2)
        hop(s, c, 6 + 4 * k, False, 1, j, 1).wait_recv()
        hop(s, c, 7 + 4 * k, False, -1, j, 2).wait_recv()
        multiply(s, c, j)

    def part_copy(i):
        return pltpu.make_async_remote_copy(
            src_ref=csend.at[i], dst_ref=crecv.at[i],
            send_sem=c_send.at[i], recv_sem=c_recv.at[i],
            device_id={"zl": 1 - zl}, device_id_type=MESH,
        )

    def fold(i):
        part_copy(i).wait_recv()
        acc[4 + i] += decode(crecv[i])

    place = (zh * 4 + y) * 4 + x

    def power_copy(d):
        dz, dy, dx = d // 16, d // 4 % 4, d % 4
        return pltpu.make_async_remote_copy(
            src_ref=sums.at[place], dst_ref=sums.at[place],
            send_sem=n_send.at[d], recv_sem=n_recv.at[d],
            device_id={
                "zh": lax.rem(zh + dz, 2), "y": lax.rem(y + dy, 4), "x": lax.rem(x + dx, 4)
            },
            device_id_type=MESH,
        )

    def out_copy(half):
        return pltpu.make_async_copy(
            acc.at[pl.ds(4 + 2 * half, 2)], out.at[pl.ds(2 * half, 2)], local_sem.at[2 + half]
        )

    def square(i):
        u = acc[4 + i]
        u = u * u
        t = u[:, :128]
        for j in range(1, u.shape[1] // 128):
            t = t + u[:, j * 128:(j + 1) * 128]
        sums[place, i] = jnp.sum(t.T, axis=0)

    @pl.loop(0, STAGES + 2)
    def _(r):
        new, mid, old = r, r - 1, r - 2
        starts = r < STAGES
        passes = jnp.logical_and(r >= 1, r < STAGES + 1)
        ends = r >= 2

        @pl.when(starts)
        def _():
            begin(new)

        @pl.when(jnp.logical_and(r == 1, jnp.logical_not(inner)))
        def _():
            for sub in range(2):
                for c in range(2):
                    for p in range(2):
                        pltpu.make_async_copy(
                            left.at[sub, c, HALVES[p]], buf.at[2 + sub, mine, c, HALVES[p]],
                            z_recv.at[2 + sub, c, p],
                        ).start()
            for c in range(2):
                for p in range(2):
                    z_copy(0, c, p, 2, 1 - zh, 0).start()

        @pl.when(jnp.logical_and(r == 2, jnp.logical_not(inner)))
        def _():
            for c in range(2):
                for p in range(2):
                    z_copy(1, c, p, 3, 1 - zh, 0).start()

        @pl.when(r == 0)
        def _():
            own_b.wait()
            own_m.wait()
            other_b.wait_recv()

        @pl.when(passes)
        def _():
            first_far(mid, 0)
            for c in range(2):
                second_near(mid, c, 0)
            first_far(mid, 1)

        @pl.when(ends)
        def _():
            for k in (2, 1, 0):
                for c in range(2):
                    second_far(old, c, k)

        @pl.when(r == STAGES + 1)
        def _():
            fold(2)
            fold(3)

        @pl.when(ends)
        def _():
            for c in range(2):
                second_far(old, c, 3)

        @pl.when(jnp.logical_and(ends, r < 4))
        def _():
            for c in range(2):
                csend[2 * old + c] = encode(acc[2 * old + c])
            for c in range(2):
                part_copy(2 * old + c).start()

        @pl.when(starts)
        def _():
            for c in range(2):
                multiply(new, c, mine)
            for c in range(2):
                first_near(new, c)

        @pl.when(passes)
        def _():
            for k in (2, 1, 3):
                for c in range(2):
                    second_near(mid, c, k)

        @pl.when(r == STAGES)
        def _():
            for i in range(2):
                fold(i)
                square(i)
            out_copy(0).start()

    for i in (2, 3):
        square(i)
    out_copy(1).start()
    for d in range(31, 0, -1):
        power_copy(d).start()
    for d in range(1, 32):
        power_copy(d).wait_recv()
    total = sums[0]
    for d in range(1, 32):
        total = total + sums[d]
    power[...] = total

    for d in range(1, 32):
        power_copy(d).wait_send()
    for i in range(4):
        part_copy(i).wait_send()
    other_b.wait_send()

    @pl.when(inner)
    def _():
        for sub in range(2):
            for c in range(2):
                for p in range(2):
                    z_copy(sub, c, p, sub, 0, 0).wait_send()
                    z_copy(sub, c, p, sub, 1, 1).wait_send()

    @pl.when(jnp.logical_not(inner))
    def _():
        for sub in range(2):
            for c in range(2):
                for p in range(2):
                    z_copy(sub, c, p, 2 + sub, 1 - zh, 0).wait_send()

    @pl.loop(0, STAGES)
    def _(s):
        for c in range(2):
            for e in range(20):
                far = e % 4 >= 2
                hop(s, c, e, True, 1, mine, 1 if far else 0).wait_send()
    out_copy(0).wait()
    out_copy(1).wait()


def body(left_factor, right_factor, matrix, pivot_scale):
    columns = matrix.shape[1]
    dma = pltpu.SemaphoreType.DMA
    updated, power = pl.pallas_call(
        kernel,
        out_shape=(
            jax.ShapeDtypeStruct((4, R, columns), jnp.float32),
            jax.ShapeDtypeStruct((4, R), jnp.float32),
        ),
        in_specs=[pl.BlockSpec(memory_space=pl.ANY)] * 4,
        out_specs=(pl.BlockSpec(memory_space=pl.ANY), pl.BlockSpec(memory_space=pltpu.VMEM)),
        scratch_shapes=[
            pltpu.VMEM((2, 2, R, DEPTH), jnp.bfloat16),
            pltpu.VMEM((64, 128), jnp.float32),
            pltpu.VMEM((2, 2, R, DEPTH), jnp.bfloat16),
            pltpu.VMEM((STAGES, 16, 2, R, DEPTH), jnp.bfloat16),
            pltpu.VMEM((16, DEPTH, columns), jnp.bfloat16),
            pltpu.VMEM((8, R, columns), jnp.float32),
            pltpu.VMEM((4, R, columns), jnp.bfloat16),
            pltpu.VMEM((4, R, columns), jnp.bfloat16),
            pltpu.VMEM((32, 4, R), jnp.float32),
            dma((STAGES, 2, 20)),
            dma((STAGES, 2, 20)),
            dma((2, 2, 2, 2)),
            dma((STAGES, 2, 2)),
            dma((4,)),
            dma((4,)),
            dma((32,)),
            dma((32,)),
            dma,
            dma,
            dma((6,)),
        ],
        compiler_params=pltpu.CompilerParams(collective_id=0, has_side_effects=True, vmem_limit_bytes=46 * 2**20),
        name="update",
    )(
        pltpu.with_memory_space_constraint(left_factor.reshape(2, 2, R, DEPTH), pltpu.HBM),
        pltpu.with_memory_space_constraint(pivot_scale.reshape(64, 128), pltpu.HBM),
        right_factor.reshape(8, DEPTH, columns),
        matrix.reshape(4, R, columns),
    )
    updated = updated.reshape(matrix.shape)
    row_power = power.reshape(matrix.shape[0])
    return updated * lax.rsqrt(row_power / (columns * 32) + 1e-06)[:, None]


def solution(mesh):
    torus = Mesh(mesh.devices.reshape(2, 2, 2, 4, 4), ROW + COL)
    in_specs = (P(ROW, COL), P(ROW, COL), P(ROW, COL), P())
    return jax.shard_map(body, mesh=torus, in_specs=in_specs, out_specs=P(ROW, COL), check_vma=False)
```

```python
import jax
import jax.numpy as jnp
from jax import lax
from jax.experimental import pallas as pl
from jax.experimental.pallas import tpu as pltpu
from jax.sharding import Mesh
from jax.sharding import PartitionSpec as P

MESH = pl.DeviceIdType.MESH
ROW = ("zl", "core")
COL = ("zh", "y", "x")
STAGES = 4
R = 256
HALF = R // 2
DEPTH = 256
HALVES = (pl.ds(0, HALF), pl.ds(HALF, HALF))
OFFSETS = (0, -1, 1, 2)


def encode(v):
    t = v * 16.0
    t2 = t * t
    t4 = t2 * t2
    t8 = t4 * t4
    return jnp.where(t < 0.0, -t8, t8).astype(jnp.bfloat16)


def decode(c):
    y = c.astype(jnp.float32)
    r = jnp.exp2(jnp.log2(jnp.abs(y)) * 0.125 - 4.0)
    return jnp.where(y < 0.0, -r, r)


def kernel(
    raw, scales, right, matrix, out, power,
    fresh_left, scale_rows, left, buf, bk, acc, csend, crecv, sums,
    send_sem, recv_sem, z_send, z_recv, c_send, c_recv, n_send, n_recv, b_send, b_recv, local_sem,
):
    x, y = lax.axis_index("x"), lax.axis_index("y")
    zl, zh, core = lax.axis_index("zl"), lax.axis_index("zh"), lax.axis_index("core")
    at = {"x": x, "y": y}
    mine = y * 4 + x

    own_b = pltpu.make_async_copy(right, bk.at[pl.ds(core * 8, 8)], local_sem.at[0])
    own_m = pltpu.make_async_copy(matrix, acc.at[pl.ds(4, 4)], local_sem.at[1])
    own_left = pltpu.make_async_copy(raw, fresh_left, local_sem.at[4])
    own_scales = pltpu.make_async_copy(scales, scale_rows, local_sem.at[5])
    own_left.start()
    own_scales.start()
    own_b.start()
    own_m.start()

    barrier = pltpu.get_barrier_semaphore()
    peers = [{"core": 1 - core}]
    for d in (1, 3):
        peers.append({"x": lax.rem(x + d, 4)})
        peers.append({"y": lax.rem(y + d, 4)})
        z = lax.rem(2 * zh + zl + d, 4)
        peers.append({"zh": z // 2, "zl": lax.rem(z, 2)})
    for peer in peers:
        pl.semaphore_signal(barrier, inc=1, device_id=peer, device_id_type=MESH)
    for i in range(4):
        acc[i] = jnp.zeros((R, acc.shape[2]), jnp.float32)
    own_scales.wait()
    own_left.wait()
    chunk = (zh * 16 + mine) * 2
    for part in range(2):
        columns = slice(part * 128, (part + 1) * 128)
        scale = scale_rows[pl.ds(chunk + part, 1), :]
        for sub in range(2):
            for c in range(2):
                left[sub, c, :, columns] = (
                    fresh_left[sub, c, :, columns].astype(jnp.float32) * scale
                ).astype(jnp.bfloat16)
    pl.semaphore_wait(barrier, len(peers))

    def z_copy(sub, c, p, stage, zh_to, k):
        return pltpu.make_async_remote_copy(
            src_ref=left.at[sub, c, HALVES[p]], dst_ref=buf.at[stage, mine, c, HALVES[p]],
            send_sem=z_send.at[k, sub, c, p], recv_sem=z_recv.at[stage, c, p],
            device_id={"zl": zh, "zh": zh_to}, device_id_type=MESH,
        )

    inner = zh != zl

    @pl.when(inner)
    def _():
        for sub in range(2):
            for c in range(2):
                for p in range(2):
                    z_copy(sub, c, p, sub, 0, 0).start()
                    z_copy(sub, c, p, sub, 1, 1).start()

    other_b = pltpu.make_async_remote_copy(
        src_ref=right, dst_ref=bk.at[pl.ds(core * 8, 8)],
        send_sem=b_send, recv_sem=b_recv, device_id={"core": 1 - core}, device_id_type=MESH,
    )
    other_b.start()

    def spot(c, dp, ds):
        px, py = (dp, ds) if c == 0 else (ds, dp)
        return lax.rem(y + py + 4, 4) * 4 + lax.rem(x + px + 4, 4)

    def hop(s, c, event, first, step, j, part):
        axis = "xy"[c] if first else "xy"[1 - c]
        rows = (slice(None), pl.ds(0, HALF), pl.ds(HALF, HALF))[part]
        piece = buf.at[s, j, c, rows]
        return pltpu.make_async_remote_copy(
            src_ref=piece, dst_ref=piece,
            send_sem=send_sem.at[s, c, event], recv_sem=recv_sem.at[s, c, event],
            device_id={axis: lax.rem(at[axis] + step + 4, 4)}, device_id_type=MESH,
        )

    def multiply(s, c, j):
        acc[2 * s + c] -= jnp.dot(buf[s, j, c], bk[j], preferred_element_type=jnp.float32)

    def send_column(s, c, k):
        j = spot(c, OFFSETS[k], 0)
        hop(s, c, 4 + 4 * k, False, 1, j, 0).start()
        hop(s, c, 5 + 4 * k, False, -1, j, 0).start()

    def begin(s):
        for c in range(2):
            for p in range(2):
                pltpu.make_async_copy(
                    left.at[0, 0, HALVES[0]], buf.at[s, mine, c, HALVES[p]], z_recv.at[s, c, p]
                ).wait()
                hop(s, c, 0, True, 1, mine, 1 + p).start()
                hop(s, c, 1, True, -1, mine, 1 + p).start()
                hop(s, c, 4, False, 1, mine, 1 + p).start()
                hop(s, c, 5, False, -1, mine, 1 + p).start()

    def first_near(s, c):
        for e, step in ((0, 1), (1, -1)):
            j = spot(c, -step, 0)
            hop(s, c, e, True, step, j, 0).wait_recv()
            hop(s, c, 2 + e, True, step, j, 1 + e).start()
            send_column(s, c, 1 + e)
            multiply(s, c, j)

    def first_far(s, c):
        j = spot(c, 2, 0)
        hop(s, c, 2, True, 1, j, 1).wait_recv()
        hop(s, c, 3, True, -1, j, 2).wait_recv()
        send_column(s, c, 3)
        multiply(s, c, j)

    def second_near(s, c, k):
        for e, step in ((0, 1), (1, -1)):
            j = spot(c, OFFSETS[k], -step)
            hop(s, c, 4 + 4 * k + e, False, step, j, 0).wait_recv()
            hop(s, c, 6 + 4 * k + e, False, step, j, 1 + e).start()
            multiply(s, c, j)

    def second_far(s, c, k):
        j = spot(c, OFFSETS[k], 2)
        hop(s, c, 6 + 4 * k, False, 1, j, 1).wait_recv()
        hop(s, c, 7 + 4 * k, False, -1, j, 2).wait_recv()
        multiply(s, c, j)

    def part_copy(i):
        return pltpu.make_async_remote_copy(
            src_ref=csend.at[i], dst_ref=crecv.at[i],
            send_sem=c_send.at[i], recv_sem=c_recv.at[i],
            device_id={"zl": 1 - zl}, device_id_type=MESH,
        )

    def fold(i):
        part_copy(i).wait_recv()
        acc[4 + i] += decode(crecv[i])

    place = (zh * 4 + y) * 4 + x

    def power_copy(d):
        dz, dy, dx = d // 16, d // 4 % 4, d % 4
        return pltpu.make_async_remote_copy(
            src_ref=sums.at[place], dst_ref=sums.at[place],
            send_sem=n_send.at[d], recv_sem=n_recv.at[d],
            device_id={
                "zh": lax.rem(zh + dz, 2), "y": lax.rem(y + dy, 4), "x": lax.rem(x + dx, 4)
            },
            device_id_type=MESH,
        )

    def out_copy(half):
        return pltpu.make_async_copy(
            acc.at[pl.ds(4 + 2 * half, 2)], out.at[pl.ds(2 * half, 2)], local_sem.at[2 + half]
        )

    def square(i):
        u = acc[4 + i]
        u = u * u
        t = u[:, :128]
        for j in range(1, u.shape[1] // 128):
            t = t + u[:, j * 128:(j + 1) * 128]
        sums[place, i] = jnp.sum(t.T, axis=0)

    @pl.loop(0, STAGES + 2)
    def _(r):
        new, mid, old = r, r - 1, r - 2
        starts = r < STAGES
        passes = jnp.logical_and(r >= 1, r < STAGES + 1)
        ends = r >= 2

        @pl.when(starts)
        def _():
            begin(new)

        @pl.when(jnp.logical_and(r == 1, jnp.logical_not(inner)))
        def _():
            for sub in range(2):
                for c in range(2):
                    for p in range(2):
                        pltpu.make_async_copy(
                            left.at[sub, c, HALVES[p]], buf.at[2 + sub, mine, c, HALVES[p]],
                            z_recv.at[2 + sub, c, p],
                        ).start()
            for c in range(2):
                for p in range(2):
                    z_copy(0, c, p, 2, 1 - zh, 0).start()

        @pl.when(jnp.logical_and(r == 2, jnp.logical_not(inner)))
        def _():
            for c in range(2):
                for p in range(2):
                    z_copy(1, c, p, 3, 1 - zh, 0).start()

        @pl.when(r == 0)
        def _():
            own_b.wait()
            own_m.wait()
            other_b.wait_recv()

        @pl.when(passes)
        def _():
            first_far(mid, 0)
            second_near(mid, 0, 0)
            second_near(mid, 1, 0)
            first_far(mid, 1)

        @pl.when(ends)
        def _():
            second_far(old, 1, 2)
            second_far(old, 0, 2)
            second_far(old, 0, 1)
            second_far(old, 1, 1)
            second_far(old, 0, 0)
            second_far(old, 1, 0)

        @pl.when(r == STAGES + 1)
        def _():
            fold(2)
            fold(3)

        @pl.when(ends)
        def _():
            second_far(old, 0, 3)
            second_far(old, 1, 3)

        @pl.when(jnp.logical_and(ends, r < 4))
        def _():
            for c in range(2):
                csend[2 * old + c] = encode(acc[2 * old + c])
            for c in range(2):
                part_copy(2 * old + c).start()

        @pl.when(starts)
        def _():
            multiply(new, 0, mine)
            first_near(new, 0)
            multiply(new, 1, mine)
            first_near(new, 1)

        @pl.when(passes)
        def _():
            second_near(mid, 0, 2)
            second_near(mid, 1, 2)
            second_near(mid, 0, 1)
            second_near(mid, 1, 1)
            second_near(mid, 0, 3)
            second_near(mid, 1, 3)

        @pl.when(r == STAGES)
        def _():
            for i in range(2):
                fold(i)
                square(i)
            out_copy(0).start()

    for i in (2, 3):
        square(i)
    out_copy(1).start()
    for d in sorted(range(1, 32), key=lambda d: -sum((d // 16 * 2, min(d // 4 % 4, 4 - d // 4 % 4), min(d % 4, 4 - d % 4)))):
        power_copy(d).start()
    for d in range(1, 32):
        power_copy(d).wait_recv()
    total = sums[0]
    for d in range(1, 32):
        total = total + sums[d]
    power[...] = total

    for d in range(1, 32):
        power_copy(d).wait_send()
    for i in range(4):
        part_copy(i).wait_send()
    other_b.wait_send()

    @pl.when(inner)
    def _():
        for sub in range(2):
            for c in range(2):
                for p in range(2):
                    z_copy(sub, c, p, sub, 0, 0).wait_send()
                    z_copy(sub, c, p, sub, 1, 1).wait_send()

    @pl.when(jnp.logical_not(inner))
    def _():
        for sub in range(2):
            for c in range(2):
                for p in range(2):
                    z_copy(sub, c, p, 2 + sub, 1 - zh, 0).wait_send()

    @pl.loop(0, STAGES)
    def _(s):
        for c in range(2):
            for e in range(20):
                far = e % 4 >= 2
                hop(s, c, e, True, 1, mine, 1 if far else 0).wait_send()
    out_copy(0).wait()
    out_copy(1).wait()


def body(left_factor, right_factor, matrix, pivot_scale):
    columns = matrix.shape[1]
    dma = pltpu.SemaphoreType.DMA
    updated, power = pl.pallas_call(
        kernel,
        out_shape=(
            jax.ShapeDtypeStruct((4, R, columns), jnp.float32),
            jax.ShapeDtypeStruct((4, R), jnp.float32),
        ),
        in_specs=[pl.BlockSpec(memory_space=pl.ANY)] * 4,
        out_specs=(pl.BlockSpec(memory_space=pl.ANY), pl.BlockSpec(memory_space=pltpu.VMEM)),
        scratch_shapes=[
            pltpu.VMEM((2, 2, R, DEPTH), jnp.bfloat16),
            pltpu.VMEM((64, 128), jnp.float32),
            pltpu.VMEM((2, 2, R, DEPTH), jnp.bfloat16),
            pltpu.VMEM((STAGES, 16, 2, R, DEPTH), jnp.bfloat16),
            pltpu.VMEM((16, DEPTH, columns), jnp.bfloat16),
            pltpu.VMEM((8, R, columns), jnp.float32),
            pltpu.VMEM((4, R, columns), jnp.bfloat16),
            pltpu.VMEM((4, R, columns), jnp.bfloat16),
            pltpu.VMEM((32, 4, R), jnp.float32),
            dma((STAGES, 2, 20)),
            dma((STAGES, 2, 20)),
            dma((2, 2, 2, 2)),
            dma((STAGES, 2, 2)),
            dma((4,)),
            dma((4,)),
            dma((32,)),
            dma((32,)),
            dma,
            dma,
            dma((6,)),
        ],
        compiler_params=pltpu.CompilerParams(collective_id=0, has_side_effects=True, vmem_limit_bytes=46 * 2**20),
        name="update",
    )(
        pltpu.with_memory_space_constraint(left_factor.reshape(2, 2, R, DEPTH), pltpu.HBM),
        pltpu.with_memory_space_constraint(pivot_scale.reshape(64, 128), pltpu.HBM),
        right_factor.reshape(8, DEPTH, columns),
        matrix.reshape(4, R, columns),
    )
    updated = updated.reshape(matrix.shape)
    row_power = power.reshape(matrix.shape[0])
    return updated * lax.rsqrt(row_power / (columns * 32) + 1e-06)[:, None]


def solution(mesh):
    torus = Mesh(mesh.devices.reshape(2, 2, 2, 4, 4), ROW + COL)
    in_specs = (P(ROW, COL), P(ROW, COL), P(ROW, COL), P())
    return jax.shard_map(body, mesh=torus, in_specs=in_specs, out_specs=P(ROW, COL), check_vma=False)
```

```python
import jax
import jax.numpy as jnp
from jax import lax
from jax.experimental import pallas as pl
from jax.experimental.pallas import tpu as pltpu
from jax.sharding import Mesh
from jax.sharding import PartitionSpec as P

MESH = pl.DeviceIdType.MESH
ROW = ("zl", "core")
COL = ("zh", "y", "x")
STAGES = 4
R = 256
HALF = R // 2
DEPTH = 256
HALVES = (pl.ds(0, HALF), pl.ds(HALF, HALF))
OFFSETS = (0, -1, 1, 2)


def encode(v):
    t = v * 16.0
    t2 = t * t
    t4 = t2 * t2
    t8 = t4 * t4
    return jnp.where(t < 0.0, -t8, t8).astype(jnp.bfloat16)


def decode(c):
    y = c.astype(jnp.float32)
    r = jnp.exp2(jnp.log2(jnp.abs(y)) * 0.125 - 4.0)
    return jnp.where(y < 0.0, -r, r)


def kernel(
    raw, scales, right, matrix, out, power,
    fresh_left, scale_rows, left, buf, bk, acc, csend, crecv, sums,
    send_sem, recv_sem, z_send, z_recv, c_send, c_recv, n_send, n_recv, b_send, b_recv, local_sem,
):
    x, y = lax.axis_index("x"), lax.axis_index("y")
    zl, zh, core = lax.axis_index("zl"), lax.axis_index("zh"), lax.axis_index("core")
    at = {"x": x, "y": y}
    mine = y * 4 + x

    own_b = pltpu.make_async_copy(right, bk.at[pl.ds(core * 8, 8)], local_sem.at[0])
    own_m = pltpu.make_async_copy(matrix, acc.at[pl.ds(4, 4)], local_sem.at[1])
    own_left = pltpu.make_async_copy(raw, fresh_left, local_sem.at[4])
    own_scales = pltpu.make_async_copy(scales, scale_rows, local_sem.at[5])
    own_left.start()
    own_scales.start()
    own_b.start()
    own_m.start()

    barrier = pltpu.get_barrier_semaphore()
    peers = [{"core": 1 - core}]
    for d in (1, 3):
        peers.append({"x": lax.rem(x + d, 4)})
        peers.append({"y": lax.rem(y + d, 4)})
        z = lax.rem(2 * zh + zl + d, 4)
        peers.append({"zh": z // 2, "zl": lax.rem(z, 2)})
    for peer in peers:
        pl.semaphore_signal(barrier, inc=1, device_id=peer, device_id_type=MESH)
    for i in range(4):
        acc[i] = jnp.zeros((R, acc.shape[2]), jnp.float32)
    own_scales.wait()
    own_left.wait()
    chunk = (zh * 16 + mine) * 2
    for part in range(2):
        columns = slice(part * 128, (part + 1) * 128)
        scale = scale_rows[pl.ds(chunk + part, 1), :]
        for sub in range(2):
            for c in range(2):
                left[sub, c, :, columns] = (
                    fresh_left[sub, c, :, columns].astype(jnp.float32) * scale
                ).astype(jnp.bfloat16)
    pl.semaphore_wait(barrier, len(peers))

    def z_copy(sub, c, p, stage, zh_to, k):
        return pltpu.make_async_remote_copy(
            src_ref=left.at[sub, c, HALVES[p]], dst_ref=buf.at[stage, mine, c, HALVES[p]],
            send_sem=z_send.at[k, sub, c, p], recv_sem=z_recv.at[stage, c, p],
            device_id={"zl": zh, "zh": zh_to}, device_id_type=MESH,
        )

    inner = zh != zl

    @pl.when(inner)
    def _():
        for sub in range(2):
            for c in range(2):
                for p in range(2):
                    z_copy(sub, c, p, sub, 0, 0).start()
                    z_copy(sub, c, p, sub, 1, 1).start()

    other_b = pltpu.make_async_remote_copy(
        src_ref=right, dst_ref=bk.at[pl.ds(core * 8, 8)],
        send_sem=b_send, recv_sem=b_recv, device_id={"core": 1 - core}, device_id_type=MESH,
    )
    other_b.start()

    def spot(c, dp, ds):
        px, py = (dp, ds) if c == 0 else (ds, dp)
        return lax.rem(y + py + 4, 4) * 4 + lax.rem(x + px + 4, 4)

    def hop(s, c, event, first, step, j, part):
        axis = "xy"[c] if first else "xy"[1 - c]
        rows = (slice(None), pl.ds(0, HALF), pl.ds(HALF, HALF))[part]
        piece = buf.at[s, j, c, rows]
        return pltpu.make_async_remote_copy(
            src_ref=piece, dst_ref=piece,
            send_sem=send_sem.at[s, c, event], recv_sem=recv_sem.at[s, c, event],
            device_id={axis: lax.rem(at[axis] + step + 4, 4)}, device_id_type=MESH,
        )

    def multiply(s, c, j):
        acc[2 * s + c] -= jnp.dot(buf[s, j, c], bk[j], preferred_element_type=jnp.float32)

    def send_column(s, c, k):
        j = spot(c, OFFSETS[k], 0)
        hop(s, c, 4 + 4 * k, False, 1, j, 0).start()
        hop(s, c, 5 + 4 * k, False, -1, j, 0).start()

    def begin(s):
        for c in range(2):
            for p in range(2):
                pltpu.make_async_copy(
                    left.at[0, 0, HALVES[0]], buf.at[s, mine, c, HALVES[p]], z_recv.at[s, c, p]
                ).wait()
                hop(s, c, 0, True, 1, mine, 1 + p).start()
                hop(s, c, 1, True, -1, mine, 1 + p).start()
                hop(s, c, 4, False, 1, mine, 1 + p).start()
                hop(s, c, 5, False, -1, mine, 1 + p).start()

    def first_near(s, c):
        for e, step in ((0, 1), (1, -1)):
            j = spot(c, -step, 0)
            hop(s, c, e, True, step, j, 0).wait_recv()
            hop(s, c, 2 + e, True, step, j, 1 + e).start()
            send_column(s, c, 1 + e)
            multiply(s, c, j)

    def first_far(s, c):
        j = spot(c, 2, 0)
        hop(s, c, 2, True, 1, j, 1).wait_recv()
        hop(s, c, 3, True, -1, j, 2).wait_recv()
        send_column(s, c, 3)
        multiply(s, c, j)

    def second_near(s, c, k):
        for e, step in ((0, 1), (1, -1)):
            j = spot(c, OFFSETS[k], -step)
            hop(s, c, 4 + 4 * k + e, False, step, j, 0).wait_recv()
            hop(s, c, 6 + 4 * k + e, False, step, j, 1 + e).start()
            multiply(s, c, j)

    def second_far(s, c, k):
        j = spot(c, OFFSETS[k], 2)
        hop(s, c, 6 + 4 * k, False, 1, j, 1).wait_recv()
        hop(s, c, 7 + 4 * k, False, -1, j, 2).wait_recv()
        multiply(s, c, j)

    def part_copy(i):
        return pltpu.make_async_remote_copy(
            src_ref=csend.at[i], dst_ref=crecv.at[i],
            send_sem=c_send.at[i], recv_sem=c_recv.at[i],
            device_id={"zl": 1 - zl}, device_id_type=MESH,
        )

    def fold(i):
        part_copy(i).wait_recv()
        acc[4 + i] += decode(crecv[i])

    place = (zh * 4 + y) * 4 + x

    def power_copy(d):
        dz, dy, dx = d // 16, d // 4 % 4, d % 4
        return pltpu.make_async_remote_copy(
            src_ref=sums.at[place], dst_ref=sums.at[place],
            send_sem=n_send.at[d], recv_sem=n_recv.at[d],
            device_id={
                "zh": lax.rem(zh + dz, 2), "y": lax.rem(y + dy, 4), "x": lax.rem(x + dx, 4)
            },
            device_id_type=MESH,
        )

    def out_copy(half):
        return pltpu.make_async_copy(
            acc.at[pl.ds(4 + 2 * half, 2)], out.at[pl.ds(2 * half, 2)], local_sem.at[2 + half]
        )

    def square(i):
        u = acc[4 + i]
        u = u * u
        t = u[:, :128]
        for j in range(1, u.shape[1] // 128):
            t = t + u[:, j * 128:(j + 1) * 128]
        sums[place, i] = jnp.sum(t.T, axis=0)

    @pl.loop(0, STAGES + 2)
    def _(r):
        new, mid, old = r, r - 1, r - 2
        starts = r < STAGES
        passes = jnp.logical_and(r >= 1, r < STAGES + 1)
        ends = r >= 2

        @pl.when(starts)
        def _():
            begin(new)

        @pl.when(jnp.logical_and(r == 1, jnp.logical_not(inner)))
        def _():
            for sub in range(2):
                for c in range(2):
                    for p in range(2):
                        pltpu.make_async_copy(
                            left.at[sub, c, HALVES[p]], buf.at[2 + sub, mine, c, HALVES[p]],
                            z_recv.at[2 + sub, c, p],
                        ).start()
            for c in range(2):
                for p in range(2):
                    z_copy(0, c, p, 2, 1 - zh, 0).start()

        @pl.when(jnp.logical_and(r == 2, jnp.logical_not(inner)))
        def _():
            for c in range(2):
                for p in range(2):
                    z_copy(1, c, p, 3, 1 - zh, 0).start()

        @pl.when(r == 0)
        def _():
            own_b.wait()
            own_m.wait()
            other_b.wait_recv()

        @pl.when(passes)
        def _():
            first_far(mid, 0)
            second_near(mid, 0, 0)
            second_near(mid, 1, 0)
            first_far(mid, 1)

        @pl.when(ends)
        def _():
            second_far(old, 1, 2)
            second_far(old, 0, 2)
            second_far(old, 0, 1)
            second_far(old, 1, 1)
            second_far(old, 0, 0)
            second_far(old, 1, 0)

        @pl.when(ends)
        def _():
            second_far(old, 0, 3)
            second_far(old, 1, 3)

        @pl.when(jnp.logical_and(ends, r < 4))
        def _():
            for c in range(2):
                csend[2 * old + c] = encode(acc[2 * old + c])
            for c in range(2):
                part_copy(2 * old + c).start()

        @pl.when(starts)
        def _():
            multiply(new, 0, mine)
            first_near(new, 0)
            multiply(new, 1, mine)
            first_near(new, 1)

        @pl.when(passes)
        def _():
            second_near(mid, 0, 2)
            second_near(mid, 1, 2)
            second_near(mid, 0, 1)
            second_near(mid, 1, 1)
            second_near(mid, 0, 3)
            second_near(mid, 1, 3)

        @pl.when(r == STAGES)
        def _():
            for i in range(2):
                fold(i)
                square(i)
            out_copy(0).start()
            fold(2)
            fold(3)

    for i in (2, 3):
        square(i)
    out_copy(1).start()
    for d in sorted(range(1, 32), key=lambda d: -sum((d // 16 * 2, min(d // 4 % 4, 4 - d // 4 % 4), min(d % 4, 4 - d % 4)))):
        power_copy(d).start()
    for d in range(1, 32):
        power_copy(d).wait_recv()
    total = sums[0]
    for d in range(1, 32):
        total = total + sums[d]
    power[...] = total

    for d in range(1, 32):
        power_copy(d).wait_send()
    for i in range(4):
        part_copy(i).wait_send()
    other_b.wait_send()

    @pl.when(inner)
    def _():
        for sub in range(2):
            for c in range(2):
                for p in range(2):
                    z_copy(sub, c, p, sub, 0, 0).wait_send()
                    z_copy(sub, c, p, sub, 1, 1).wait_send()

    @pl.when(jnp.logical_not(inner))
    def _():
        for sub in range(2):
            for c in range(2):
                for p in range(2):
                    z_copy(sub, c, p, 2 + sub, 1 - zh, 0).wait_send()

    @pl.loop(0, STAGES)
    def _(s):
        for c in range(2):
            for e in range(20):
                far = e % 4 >= 2
                hop(s, c, e, True, 1, mine, 1 if far else 0).wait_send()
    out_copy(0).wait()
    out_copy(1).wait()


def body(left_factor, right_factor, matrix, pivot_scale):
    columns = matrix.shape[1]
    dma = pltpu.SemaphoreType.DMA
    updated, power = pl.pallas_call(
        kernel,
        out_shape=(
            jax.ShapeDtypeStruct((4, R, columns), jnp.float32),
            jax.ShapeDtypeStruct((4, R), jnp.float32),
        ),
        in_specs=[pl.BlockSpec(memory_space=pl.ANY)] * 4,
        out_specs=(pl.BlockSpec(memory_space=pl.ANY), pl.BlockSpec(memory_space=pltpu.VMEM)),
        scratch_shapes=[
            pltpu.VMEM((2, 2, R, DEPTH), jnp.bfloat16),
            pltpu.VMEM((64, 128), jnp.float32),
            pltpu.VMEM((2, 2, R, DEPTH), jnp.bfloat16),
            pltpu.VMEM((STAGES, 16, 2, R, DEPTH), jnp.bfloat16),
            pltpu.VMEM((16, DEPTH, columns), jnp.bfloat16),
            pltpu.VMEM((8, R, columns), jnp.float32),
            pltpu.VMEM((4, R, columns), jnp.bfloat16),
            pltpu.VMEM((4, R, columns), jnp.bfloat16),
            pltpu.VMEM((32, 4, R), jnp.float32),
            dma((STAGES, 2, 20)),
            dma((STAGES, 2, 20)),
            dma((2, 2, 2, 2)),
            dma((STAGES, 2, 2)),
            dma((4,)),
            dma((4,)),
            dma((32,)),
            dma((32,)),
            dma,
            dma,
            dma((6,)),
        ],
        compiler_params=pltpu.CompilerParams(collective_id=0, has_side_effects=True, vmem_limit_bytes=46 * 2**20),
        name="update",
    )(
        pltpu.with_memory_space_constraint(left_factor.reshape(2, 2, R, DEPTH), pltpu.HBM),
        pltpu.with_memory_space_constraint(pivot_scale.reshape(64, 128), pltpu.HBM),
        right_factor.reshape(8, DEPTH, columns),
        matrix.reshape(4, R, columns),
    )
    updated = updated.reshape(matrix.shape)
    row_power = power.reshape(matrix.shape[0])
    return updated * lax.rsqrt(row_power / (columns * 32) + 1e-06)[:, None]


def solution(mesh):
    torus = Mesh(mesh.devices.reshape(2, 2, 2, 4, 4), ROW + COL)
    in_specs = (P(ROW, COL), P(ROW, COL), P(ROW, COL), P())
    return jax.shard_map(body, mesh=torus, in_specs=in_specs, out_specs=P(ROW, COL), check_vma=False)
```

```python
import jax
import jax.numpy as jnp
from jax import lax
from jax.experimental import pallas as pl
from jax.experimental.pallas import tpu as pltpu
from jax.sharding import Mesh
from jax.sharding import PartitionSpec as P

MESH = pl.DeviceIdType.MESH
ROW = ("zl", "core")
COL = ("zh", "y", "x")
STAGES = 4
R = 256
HALF = R // 2
DEPTH = 256
HALVES = (pl.ds(0, HALF), pl.ds(HALF, HALF))
OFFSETS = (0, -1, 1, 2)


def encode(v):
    t = v * 16.0
    t2 = t * t
    t4 = t2 * t2
    t8 = t4 * t4
    return jnp.where(t < 0.0, -t8, t8).astype(jnp.bfloat16)


def decode(c):
    y = c.astype(jnp.float32)
    r = jnp.exp2(jnp.log2(jnp.abs(y)) * 0.125 - 4.0)
    return jnp.where(y < 0.0, -r, r)


def kernel(
    raw, scales, right, matrix, out, power,
    fresh_left, scale_rows, left, buf, bk, acc, csend, crecv, sums,
    send_sem, recv_sem, z_send, z_recv, c_send, c_recv, n_send, n_recv, b_send, b_recv, local_sem,
):
    x, y = lax.axis_index("x"), lax.axis_index("y")
    zl, zh, core = lax.axis_index("zl"), lax.axis_index("zh"), lax.axis_index("core")
    at = {"x": x, "y": y}
    mine = y * 4 + x

    own_b = pltpu.make_async_copy(right, bk.at[pl.ds(core * 8, 8)], local_sem.at[0])
    own_m = pltpu.make_async_copy(matrix, acc.at[pl.ds(4, 4)], local_sem.at[1])
    own_left = pltpu.make_async_copy(raw, fresh_left, local_sem.at[4])
    own_scales = pltpu.make_async_copy(scales, scale_rows, local_sem.at[5])
    own_left.start()
    own_scales.start()
    own_b.start()
    own_m.start()

    barrier = pltpu.get_barrier_semaphore()
    peers = [{"core": 1 - core}]
    for d in (1, 3):
        peers.append({"x": lax.rem(x + d, 4)})
        peers.append({"y": lax.rem(y + d, 4)})
        z = lax.rem(2 * zh + zl + d, 4)
        peers.append({"zh": z // 2, "zl": lax.rem(z, 2)})
    for peer in peers:
        pl.semaphore_signal(barrier, inc=1, device_id=peer, device_id_type=MESH)
    for i in range(4):
        acc[i] = jnp.zeros((R, acc.shape[2]), jnp.float32)
    own_scales.wait()
    own_left.wait()
    chunk = (zh * 16 + mine) * 2
    for part in range(2):
        columns = slice(part * 128, (part + 1) * 128)
        scale = scale_rows[pl.ds(chunk + part, 1), :]
        for sub in range(2):
            for c in range(2):
                left[sub, c, :, columns] = (
                    fresh_left[sub, c, :, columns].astype(jnp.float32) * scale
                ).astype(jnp.bfloat16)
    pl.semaphore_wait(barrier, len(peers))

    def z_copy(sub, c, p, stage, zh_to, k):
        return pltpu.make_async_remote_copy(
            src_ref=left.at[sub, c, HALVES[p]], dst_ref=buf.at[stage, mine, c, HALVES[p]],
            send_sem=z_send.at[k, sub, c, p], recv_sem=z_recv.at[stage, c, p],
            device_id={"zl": zh, "zh": zh_to}, device_id_type=MESH,
        )

    inner = zh != zl

    @pl.when(inner)
    def _():
        for sub in range(2):
            for c in range(2):
                for p in range(2):
                    z_copy(sub, c, p, sub, 0, 0).start()
                    z_copy(sub, c, p, sub, 1, 1).start()

    other_b = pltpu.make_async_remote_copy(
        src_ref=right, dst_ref=bk.at[pl.ds(core * 8, 8)],
        send_sem=b_send, recv_sem=b_recv, device_id={"core": 1 - core}, device_id_type=MESH,
    )
    other_b.start()

    def spot(c, dp, ds):
        px, py = (dp, ds) if c == 0 else (ds, dp)
        return lax.rem(y + py + 4, 4) * 4 + lax.rem(x + px + 4, 4)

    def hop(s, c, event, first, step, j, part):
        axis = "xy"[c] if first else "xy"[1 - c]
        rows = (slice(None), pl.ds(0, HALF), pl.ds(HALF, HALF))[part]
        piece = buf.at[s, j, c, rows]
        return pltpu.make_async_remote_copy(
            src_ref=piece, dst_ref=piece,
            send_sem=send_sem.at[s, c, event], recv_sem=recv_sem.at[s, c, event],
            device_id={axis: lax.rem(at[axis] + step + 4, 4)}, device_id_type=MESH,
        )

    def multiply(s, c, j):
        acc[2 * s + c] -= jnp.dot(buf[s, j, c], bk[j], preferred_element_type=jnp.float32)

    def send_column(s, c, k):
        j = spot(c, OFFSETS[k], 0)
        hop(s, c, 4 + 4 * k, False, 1, j, 0).start()
        hop(s, c, 5 + 4 * k, False, -1, j, 0).start()

    def begin(s):
        for c in range(2):
            for p in range(2):
                pltpu.make_async_copy(
                    left.at[0, 0, HALVES[0]], buf.at[s, mine, c, HALVES[p]], z_recv.at[s, c, p]
                ).wait()
                hop(s, c, 0, True, 1, mine, 1 + p).start()
                hop(s, c, 1, True, -1, mine, 1 + p).start()
                hop(s, c, 4, False, 1, mine, 1 + p).start()
                hop(s, c, 5, False, -1, mine, 1 + p).start()

    def first_near(s, c):
        for e, step in ((0, 1), (1, -1)):
            j = spot(c, -step, 0)
            hop(s, c, e, True, step, j, 0).wait_recv()
            hop(s, c, 2 + e, True, step, j, 1 + e).start()
            send_column(s, c, 1 + e)
        for step in (1, -1):
            multiply(s, c, spot(c, -step, 0))

    def first_far(s, c):
        j = spot(c, 2, 0)
        hop(s, c, 2, True, 1, j, 1).wait_recv()
        hop(s, c, 3, True, -1, j, 2).wait_recv()
        send_column(s, c, 3)
        multiply(s, c, j)

    def second_near(s, c, k):
        for e, step in ((0, 1), (1, -1)):
            j = spot(c, OFFSETS[k], -step)
            hop(s, c, 4 + 4 * k + e, False, step, j, 0).wait_recv()
            hop(s, c, 6 + 4 * k + e, False, step, j, 1 + e).start()
        for step in (1, -1):
            multiply(s, c, spot(c, OFFSETS[k], -step))

    def second_far(s, c, k):
        j = spot(c, OFFSETS[k], 2)
        hop(s, c, 6 + 4 * k, False, 1, j, 1).wait_recv()
        hop(s, c, 7 + 4 * k, False, -1, j, 2).wait_recv()
        multiply(s, c, j)

    def part_copy(i):
        return pltpu.make_async_remote_copy(
            src_ref=csend.at[i], dst_ref=crecv.at[i],
            send_sem=c_send.at[i], recv_sem=c_recv.at[i],
            device_id={"zl": 1 - zl}, device_id_type=MESH,
        )

    def fold(i):
        part_copy(i).wait_recv()
        acc[4 + i] += decode(crecv[i])

    place = (zh * 4 + y) * 4 + x

    def power_copy(d):
        dz, dy, dx = d // 16, d // 4 % 4, d % 4
        return pltpu.make_async_remote_copy(
            src_ref=sums.at[place], dst_ref=sums.at[place],
            send_sem=n_send.at[d], recv_sem=n_recv.at[d],
            device_id={
                "zh": lax.rem(zh + dz, 2), "y": lax.rem(y + dy, 4), "x": lax.rem(x + dx, 4)
            },
            device_id_type=MESH,
        )

    def out_copy(half):
        return pltpu.make_async_copy(
            acc.at[pl.ds(4 + 2 * half, 2)], out.at[pl.ds(2 * half, 2)], local_sem.at[2 + half]
        )

    def square(i):
        u = acc[4 + i]
        u = u * u
        t = u[:, :128]
        for j in range(1, u.shape[1] // 128):
            t = t + u[:, j * 128:(j + 1) * 128]
        sums[place, i] = jnp.sum(t.T, axis=0)

    @pl.loop(0, STAGES + 2)
    def _(r):
        new, mid, old = r, r - 1, r - 2
        starts = r < STAGES
        passes = jnp.logical_and(r >= 1, r < STAGES + 1)
        ends = r >= 2

        @pl.when(starts)
        def _():
            begin(new)

        @pl.when(jnp.logical_and(r == 1, jnp.logical_not(inner)))
        def _():
            for sub in range(2):
                for c in range(2):
                    for p in range(2):
                        pltpu.make_async_copy(
                            left.at[sub, c, HALVES[p]], buf.at[2 + sub, mine, c, HALVES[p]],
                            z_recv.at[2 + sub, c, p],
                        ).start()
            for c in range(2):
                for p in range(2):
                    z_copy(0, c, p, 2, 1 - zh, 0).start()

        @pl.when(jnp.logical_and(r == 2, jnp.logical_not(inner)))
        def _():
            for c in range(2):
                for p in range(2):
                    z_copy(1, c, p, 3, 1 - zh, 0).start()

        @pl.when(r == 0)
        def _():
            own_b.wait()
            own_m.wait()
            other_b.wait_recv()

        @pl.when(passes)
        def _():
            first_far(mid, 0)
            second_near(mid, 0, 0)
            second_near(mid, 1, 0)
            first_far(mid, 1)

        @pl.when(ends)
        def _():
            second_far(old, 1, 2)
            second_far(old, 0, 2)
            second_far(old, 0, 1)
            second_far(old, 1, 1)
            second_far(old, 0, 0)
            second_far(old, 1, 0)

        @pl.when(r == STAGES + 1)
        def _():
            fold(2)
            fold(3)

        @pl.when(ends)
        def _():
            second_far(old, 0, 3)
            second_far(old, 1, 3)

        @pl.when(jnp.logical_and(ends, r < 4))
        def _():
            for c in range(2):
                csend[2 * old + c] = encode(acc[2 * old + c])
            for c in range(2):
                part_copy(2 * old + c).start()

        @pl.when(starts)
        def _():
            multiply(new, 0, mine)
            first_near(new, 0)
            multiply(new, 1, mine)
            first_near(new, 1)

        @pl.when(passes)
        def _():
            second_near(mid, 0, 2)
            second_near(mid, 1, 2)
            second_near(mid, 0, 1)
            second_near(mid, 1, 1)
            second_near(mid, 0, 3)
            second_near(mid, 1, 3)

        @pl.when(r == STAGES)
        def _():
            for i in range(2):
                fold(i)
                square(i)
            out_copy(0).start()

    for i in (2, 3):
        square(i)
    out_copy(1).start()
    for d in sorted(range(1, 32), key=lambda d: -sum((d // 16 * 2, min(d // 4 % 4, 4 - d // 4 % 4), min(d % 4, 4 - d % 4)))):
        power_copy(d).start()
    for d in range(1, 32):
        power_copy(d).wait_recv()
    total = sums[0]
    for d in range(1, 32):
        total = total + sums[d]
    power[...] = total

    for d in range(1, 32):
        power_copy(d).wait_send()
    for i in range(4):
        part_copy(i).wait_send()
    other_b.wait_send()

    @pl.when(inner)
    def _():
        for sub in range(2):
            for c in range(2):
                for p in range(2):
                    z_copy(sub, c, p, sub, 0, 0).wait_send()
                    z_copy(sub, c, p, sub, 1, 1).wait_send()

    @pl.when(jnp.logical_not(inner))
    def _():
        for sub in range(2):
            for c in range(2):
                for p in range(2):
                    z_copy(sub, c, p, 2 + sub, 1 - zh, 0).wait_send()

    @pl.loop(0, STAGES)
    def _(s):
        for c in range(2):
            for e in range(20):
                far = e % 4 >= 2
                hop(s, c, e, True, 1, mine, 1 if far else 0).wait_send()
    out_copy(0).wait()
    out_copy(1).wait()


def body(left_factor, right_factor, matrix, pivot_scale):
    columns = matrix.shape[1]
    dma = pltpu.SemaphoreType.DMA
    updated, power = pl.pallas_call(
        kernel,
        out_shape=(
            jax.ShapeDtypeStruct((4, R, columns), jnp.float32),
            jax.ShapeDtypeStruct((4, R), jnp.float32),
        ),
        in_specs=[pl.BlockSpec(memory_space=pl.ANY)] * 4,
        out_specs=(pl.BlockSpec(memory_space=pl.ANY), pl.BlockSpec(memory_space=pltpu.VMEM)),
        scratch_shapes=[
            pltpu.VMEM((2, 2, R, DEPTH), jnp.bfloat16),
            pltpu.VMEM((64, 128), jnp.float32),
            pltpu.VMEM((2, 2, R, DEPTH), jnp.bfloat16),
            pltpu.VMEM((STAGES, 16, 2, R, DEPTH), jnp.bfloat16),
            pltpu.VMEM((16, DEPTH, columns), jnp.bfloat16),
            pltpu.VMEM((8, R, columns), jnp.float32),
            pltpu.VMEM((4, R, columns), jnp.bfloat16),
            pltpu.VMEM((4, R, columns), jnp.bfloat16),
            pltpu.VMEM((32, 4, R), jnp.float32),
            dma((STAGES, 2, 20)),
            dma((STAGES, 2, 20)),
            dma((2, 2, 2, 2)),
            dma((STAGES, 2, 2)),
            dma((4,)),
            dma((4,)),
            dma((32,)),
            dma((32,)),
            dma,
            dma,
            dma((6,)),
        ],
        compiler_params=pltpu.CompilerParams(collective_id=0, has_side_effects=True, vmem_limit_bytes=46 * 2**20),
        name="update",
    )(
        pltpu.with_memory_space_constraint(left_factor.reshape(2, 2, R, DEPTH), pltpu.HBM),
        pltpu.with_memory_space_constraint(pivot_scale.reshape(64, 128), pltpu.HBM),
        right_factor.reshape(8, DEPTH, columns),
        matrix.reshape(4, R, columns),
    )
    updated = updated.reshape(matrix.shape)
    row_power = power.reshape(matrix.shape[0])
    return updated * lax.rsqrt(row_power / (columns * 32) + 1e-06)[:, None]


def solution(mesh):
    torus = Mesh(mesh.devices.reshape(2, 2, 2, 4, 4), ROW + COL)
    in_specs = (P(ROW, COL), P(ROW, COL), P(ROW, COL), P())
    return jax.shard_map(body, mesh=torus, in_specs=in_specs, out_specs=P(ROW, COL), check_vma=False)
```
